8 devices in a mesh: rep: 1 (over z), dp: 8 (over x, y, core).
Axes of the slice: x: 2, y: 2, z: 1, core: 2. Of those that a mesh axis runs over, the one named last changes fastest.
Arguments:
- x: bfloat16 [8, 2048, 896], P(('rep', 'dp'))
- dy: bfloat16 [8, 2048, 896], P(('rep', 'dp'))
- w_gate: bfloat16 [2, 896, 4736], replicated
- w_up: bfloat16 [2, 896, 4736], replicated
- w_down: bfloat16 [2, 4736, 896], replicated
- m_w_gate: float32 [2, 896, 4736], replicated
- m_w_up: float32 [2, 896, 4736], replicated
- m_w_down: float32 [2, 4736, 896], replicated
- v_w_gate: float32 [2, 896, 4736], replicated
- v_w_up: float32 [2, 896, 4736], replicated
- v_w_down: float32 [2, 4736, 896], replicated
Outputs:
- output 1: bfloat16 [2, 896, 4736], P('rep')
- output 2: bfloat16 [2, 896, 4736], P('rep')
- output 3: bfloat16 [2, 4736, 896], P('rep')
- output 4: float32 [2, 896, 4736], P('rep')
- output 5: float32 [2, 896, 4736], P('rep')
- output 6: float32 [2, 4736, 896], P('rep')
- output 7: float32 [2, 896, 4736], P('rep')
- output 8: float32 [2, 896, 4736], P('rep')
- output 9: float32 [2, 4736, 896], P('rep')
All inputs are finite; a program needn't handle non-finite values.
Results may differ from the reference program's by a relative error of at most 0.022.
Values are sent between devices in bfloat16 or wider.
A program may use at most 3 GiB of HBM per device.

```python
import jax
import jax.numpy as jnp
from jax import lax

SEQUENCES = 8
TOKENS = 2048
D = 896
FF = 4736
LAYERS = 2
NAMES = ("w_gate", "w_up", "w_down")
SHAPES = {"w_gate": (LAYERS, D, FF), "w_up": (LAYERS, D, FF), "w_down": (LAYERS, FF, D)}


def bump(key, n, height):
    away = (jnp.arange(n, dtype=jnp.int32) - jax.random.randint(key, (), 0, n, jnp.int32)) % n
    return jnp.where(away < n // 8, height, 1.0)


def together(key, own, strength):
    shared = jax.random.normal(key, own.shape[1:], jnp.float32)
    return (own + strength * shared) * lax.rsqrt(1 + strength * strength)


def setup_inputs(seed: int = 0, part: int = 0) -> dict:
    kx, kdy, ka, kb, kz, kf, kh, kl, *keys = jax.random.split(jax.random.key(seed), 8 + 3 * len(NAMES))
    kx, kdy, ka, kb = (jax.random.fold_in(k, part) for k in (kx, kdy, ka, kb))
    kw, km, kv = (keys[i::3] for i in range(3))
    shape = (SEQUENCES, TOKENS, D)
    much_x, much_dy = jax.random.uniform(kz, (2,), jnp.float32, 0.0, 1.0)
    loud = 2.0 ** jax.random.uniform(jax.random.fold_in(kz, 1), (), jnp.float32, -1.0, 2.0)
    layers = 2.0 ** jax.random.uniform(kl, (LAYERS, 1, 1), jnp.float32, -1.0, 1.0)
    x = together(ka, jax.random.normal(kx, shape, jnp.float32), much_x) * bump(kf, D, 4.0)
    dy = together(kb, jax.random.normal(kdy, shape, jnp.float32), much_dy)
    drawn = {"x": x.astype(jnp.bfloat16), "dy": (loud * dy * (SEQUENCES * TOKENS) ** -0.5).astype(jnp.bfloat16)}
    for key, name in zip(kw, NAMES, strict=True):
        w = jax.random.normal(key, SHAPES[name], jnp.float32) * SHAPES[name][1] ** -0.5
        drawn[name] = (w * {"w_gate": 1.0, "w_up": bump(kh, FF, 4.0), "w_down": layers}[name]).astype(jnp.bfloat16)
    for key, name in zip(km, NAMES, strict=True):
        drawn[f"m_{name}"] = 0.1 * jax.random.normal(key, SHAPES[name], jnp.float32)
    for key, name in zip(kv, NAMES, strict=True):
        drawn[f"v_{name}"] = jax.random.uniform(key, SHAPES[name], jnp.float32, 0.005, 0.015)
    return drawn


def matmul(a, w):
    return jnp.dot(a, w, preferred_element_type=jnp.float32).astype(jnp.bfloat16)


def normed(h):
    wide = h.astype(jnp.float32)
    scale = lax.rsqrt(jnp.mean(wide**2, -1, keepdims=True) + 1e-6)
    return (wide * scale).astype(jnp.bfloat16)


def layer(h, w):
    a = normed(h)
    gate = jnp.dot(a, w["w_gate"], preferred_element_type=jnp.float32)
    up = jnp.dot(a, w["w_up"], preferred_element_type=jnp.float32)
    return h + matmul((jax.nn.silu(gate) * up).astype(jnp.bfloat16), w["w_down"])


def adamw(w, m, v, g):
    m = 0.9 * m + 0.1 * g
    v = 0.95 * v + 0.05 * g * g
    step = m * lax.rsqrt(v + 1e-8) + 0.1 * w
    return (w - 0.02 * step).astype(jnp.bfloat16), m, v


def clipped(gradients, sum_of_squares, count):
    factor = jnp.minimum(1.0, 0.5 * lax.rsqrt(sum_of_squares / count + 1e-30))
    return [g * factor for g in gradients]


def stack(weights, h):
    return lax.scan(lambda h, w: (layer(h, w), None), h, weights)[0]


def reference(x, dy, w_gate, w_up, w_down, m_w_gate, m_w_up, m_w_down, v_w_gate, v_w_up, v_w_down):
    weights = dict(zip(NAMES, (w_gate, w_up, w_down), strict=True))

    def take(so_far, sequence):
        h, by_y = sequence
        _, back = jax.vjp(lambda w: stack(w, h), weights)
        return jax.tree.map(lambda total, term: total + term.astype(jnp.float32), so_far, back(by_y)[0]), None

    none_yet = {name: jnp.zeros(w.shape, jnp.float32) for name, w in weights.items()}
    by_weights, _ = lax.scan(take, none_yet, (x, dy))
    gradients = [by_weights[name].astype(jnp.bfloat16).astype(jnp.float32) for name in NAMES]
    gradients = clipped(gradients, sum(jnp.sum(g * g) for g in gradients), sum(g.size for g in gradients))
    new = [
        adamw(w.astype(jnp.float32), m, v, g)
        for w, m, v, g in zip((w_gate, w_up, w_down), (m_w_gate, m_w_up, m_w_down), (v_w_gate, v_w_up, v_w_down), gradients, strict=True)
    ]
    return tuple(one[which] for which in range(3) for one in new)
```

```python
import functools

import jax
import jax.numpy as jnp
from jax import lax
from jax.experimental import pallas as pl
from jax.experimental.pallas import tpu as pltpu
from jax.sharding import PartitionSpec as P

BF, F32 = jnp.bfloat16, jnp.float32
FC = 256
TM = 512
LIMIT = 62 * 1024 * 1024
SPREAD = 10
LAG = 2
SLOTS = 4


def normed(h):
    wide = h.astype(F32)
    scale = lax.rsqrt(jnp.mean(wide**2, -1, keepdims=True) + 1e-6)
    return (wide * scale).astype(BF)


def nt(a, b):
    return lax.dot_general(a, b, (((1,), (1,)), ((), ())), preferred_element_type=F32)


def nn(a, b):
    return jnp.dot(a, b, preferred_element_type=F32)


def masked(c, width, axis, w):
    place = lax.broadcasted_iota(jnp.int32, w.shape, axis) + c * FC
    return jnp.where(place < width, w, jnp.zeros_like(w))


def once(shape):
    return pl.BlockSpec(shape, lambda c: (0,) * len(shape), pipeline_mode=pl.Buffered(1))


def params(**more):
    return pltpu.CompilerParams(vmem_limit_bytes=LIMIT, dimension_semantics=("arbitrary",), **more)


def fwd_body(width, x_ref, wg_ref, wu_ref, wd_ref, g_ref, u_ref, h_ref, a_ref, acc, ws, wds):
    c = pl.program_id(0)

    @pl.when(c == 0)
    def _():
        acc[...] = jnp.zeros_like(acc)
        a_ref[...] = normed(x_ref[...])

    ws[:, :FC] = masked(c, width, 1, wg_ref[...])
    ws[:, FC:] = masked(c, width, 1, wu_ref[...])
    wds[...] = masked(c, width, 0, wd_ref[...])

    def tile(i, _):
        rows = pl.ds(pl.multiple_of(i * TM, TM), TM)
        gu = nn(a_ref[rows, :], ws[...])
        g, u = gu[:, :FC], gu[:, FC:]
        g_ref[rows, :] = g
        u_ref[rows, :] = u
        acc[rows, :] += nn((g * jax.nn.sigmoid(g) * u).astype(BF), wds[...])
        return 0

    lax.fori_loop(0, a_ref.shape[0] // TM, tile, 0, unroll=True)

    @pl.when(c == pl.num_programs(0) - 1)
    def _():
        h_ref[...] = x_ref[...] + acc[...].astype(BF)


def forward(layer, x, w_gate, w_up, w_down):
    t, d = x.shape
    f = w_gate.shape[2]
    n = pl.cdiv(f, FC)
    wcol = pl.BlockSpec((None, d, FC), lambda c: (layer, 0, c))
    wrow = pl.BlockSpec((None, FC, d), lambda c: (layer, c, 0))
    return pl.pallas_call(
        functools.partial(fwd_body, f),
        grid=(n,),
        in_specs=[once((t, d)), wcol, wcol, wrow],
        out_specs=[pl.BlockSpec((t, FC), lambda c: (0, c))] * 2 + [once((t, d))],
        out_shape=[jax.ShapeDtypeStruct((t, n * FC), F32)] * 2 + [jax.ShapeDtypeStruct((t, d), BF)],
        scratch_shapes=[pltpu.VMEM((t, d), BF), pltpu.VMEM((t, d), F32), pltpu.VMEM((d, 2 * FC), BF), pltpu.VMEM((FC, d), BF)],
        compiler_params=params(),
        cost_estimate=pl.CostEstimate(flops=6 * t * d * f, bytes_accessed=10 * t * f, transcendentals=t * f),
        name="forward",
    )(x, w_gate, w_up, w_down)


class Sum:
    def __init__(self, n, rows, out_ref, ss_ref, refs, spread=0, whole_ref=None):
        self.n, self.rows, self.out, self.ss = n, rows, out_ref, ss_ref
        self.spread, self.whole = spread, whole_ref
        self.own, self.land0, self.send1, self.keep1, self.land1, self.send2, self.keep2, self.land2 = refs[:8]
        self.sends, self.lands = refs[8:14:2], refs[9:14:2]
        if spread:
            self.fin, self.local, *sems = refs[14:]
            self.out_sends, self.out_lands = sems[::2], sems[1::2]
        me = self.me = lax.axis_index("dp")
        self.x, self.y, self.core = me // 4, (me // 2) % 2, me % 2
        self.over = (me + 1 - 2 * self.core, me + 4 - 8 * self.x, me + 2 - 4 * self.y)

    @staticmethod
    def scratch(rows):
        def buffer(slots, *shape, dtype=BF):
            return pltpu.VMEM((slots, *shape, rows, FC), dtype)

        return [
            buffer(2, 2, 3, 4),
            buffer(SLOTS, 3, 4),
            buffer(2, 3, 2),
            buffer(2, 3, 2, dtype=F32),
            buffer(SLOTS, 3, 2),
            buffer(2, 3),
            buffer(2, 3, dtype=F32),
            buffer(SLOTS, 3),
        ] + [pltpu.SemaphoreType.DMA((2,)), pltpu.SemaphoreType.DMA((SLOTS,))] * 3

    @staticmethod
    def spread_scratch(rows):
        sems = [pltpu.SemaphoreType.DMA((slots, copies)) for copies in (1, 2, 4) for slots in (2, SLOTS)]
        return [pltpu.VMEM((2, 3, rows, FC), BF), pltpu.SemaphoreType.DMA((2,)), *sems]

    def enter(self):
        barrier = pltpu.get_barrier_semaphore()
        for other in self.over:
            pl.semaphore_signal(barrier, inc=1, device_id={"dp": other}, device_id_type=pl.DeviceIdType.MESH)
        pl.semaphore_wait(barrier, 3)

    def put(self, c, which, g):
        slot = lax.rem(c, 2)
        for j in range(8):
            core, x, y = (j % 2 + self.core) % 2, (j // 4 + self.x) % 2, ((j // 2) % 2 + self.y) % 2
            self.own[slot, core, which, x * 2 + y] = g[j * self.rows : (j + 1) * self.rows].astype(BF)

    def copy(self, stage, k):
        two, four, odd = lax.rem(k, 2), lax.rem(k, SLOTS), lax.rem(k, 2)
        if stage == 0:
            src, dst, to = self.own.at[two, 1], self.land0.at[four], self.over[0]
        elif stage == 1:
            src, dst, to = self.send1.at[two], self.land1.at[four], self.over[1] * (1 - odd) + self.over[2] * odd
        else:
            src, dst, to = self.send2.at[two], self.land2.at[four], self.over[2] * (1 - odd) + self.over[1] * odd
        return pltpu.make_async_remote_copy(
            src_ref=src,
            dst_ref=dst,
            send_sem=self.sends[stage].at[two],
            recv_sem=self.lands[stage].at[four],
            device_id={"dp": to},
            device_id_type=pl.DeviceIdType.MESH,
        )

    def when(self, k, n=None):
        return pl.when((k >= 0) & (k < (self.n if n is None else n)))

    def keep(self, k):
        return pltpu.make_async_copy(self.fin.at[lax.rem(k, 2)], self.whole.at[self.me, k], self.local.at[lax.rem(k, 2)])

    def give(self, stage, k):
        two, four, odd = lax.rem(k, 2), lax.rem(k, SLOTS), lax.rem(k, 2)
        near = self.over[1] * (1 - odd) + self.over[2] * odd
        far = self.over[2] * (1 - odd) + self.over[1] * odd
        blocks = (self.me, far, near, near + far - self.me)[: 2**stage]
        to = (far, near, self.over[0])[stage]
        return [
            pltpu.make_async_remote_copy(
                src_ref=self.whole.at[block, k] if stage else self.fin.at[two],
                dst_ref=self.whole.at[block, k],
                send_sem=self.out_sends[stage].at[two, i],
                recv_sem=self.out_lands[stage].at[four, i],
                device_id={"dp": to},
                device_id_type=pl.DeviceIdType.MESH,
            )
            for i, block in enumerate(blocks)
        ]

    def receive(self, c):
        for stage in (2, 1, 0) if self.spread else ():
            k = c - (4 + stage) * LAG

            @self.when(k, self.spread)
            def _(stage=stage, k=k):
                if stage == 0:
                    self.keep(k).wait()
                for copy in self.give(stage, k):
                    copy.wait()

        k2 = c - 3 * LAG

        @self.when(k2)
        def _():
            self.copy(2, k2).wait()
            g = (self.keep2[lax.rem(k2, 2)] + self.land2[lax.rem(k2, SLOTS)].astype(F32)).astype(BF)
            self.out[...] = g
            if self.spread:
                self.fin[lax.rem(k2, 2)] = g
            g = g.astype(F32)
            self.ss[...] += g[0] * g[0] + g[1] * g[1] + g[2] * g[2]

        k1 = c - 2 * LAG

        @self.when(k1)
        def _():
            self.copy(1, k1).wait()
            two, four = lax.rem(k1, 2), lax.rem(k1, SLOTS)
            self.keep2[two] = self.keep1[two, :, 0] + self.land1[four, :, 0].astype(F32)
            self.send2[two] = (self.keep1[two, :, 1] + self.land1[four, :, 1].astype(F32)).astype(BF)

        k0 = c - LAG

        @self.when(k0)
        def _():
            self.copy(0, k0).wait()
            two, four = lax.rem(k0, 2), lax.rem(k0, SLOTS)
            odd = two
            for to, place in ((0, 0), (1, 1 + odd)):
                self.keep1[two, :, to] = self.own[two, 0, :, place].astype(F32) + self.land0[four, :, place].astype(F32)
            for to, place in ((0, 2 - odd), (1, 3)):
                self.send1[two, :, to] = (self.own[two, 0, :, place].astype(F32) + self.land0[four, :, place].astype(F32)).astype(BF)

    def send(self, c):
        for stage in range(3):
            k = c - stage * LAG

            @self.when(k)
            def _(stage=stage, k=k):
                self.copy(stage, k).start()

        for stage in range(3 if self.spread else 0):
            k = c - (3 + stage) * LAG

            @self.when(k, self.spread)
            def _(stage=stage, k=k):
                if stage == 0:
                    self.keep(k).start()
                for copy in self.give(stage, k):
                    copy.start()


def back(g, u, dh):
    s = jax.nn.sigmoid(g)
    silu = g * s
    return (silu * u).astype(BF), (dh * u * (s + silu * (1 - s))).astype(BF), (dh * silu).astype(BF)


def gradients(total, c, at_ref, dyt_ref, dgu, hid):
    o = nn(at_ref[...], dgu[...])
    total.put(c, 0, o[:, :FC])
    total.put(c, 1, o[:, FC:])
    total.put(c, 2, nn(dyt_ref[...], hid[...]))


def turn(to_ref, of):
    for i in range(to_ref.shape[1] // TM):
        rows = pl.ds(i * TM, TM)
        to_ref[:, rows] = of(rows).T


def by_normed(h, by_a):
    h, by_a = h.astype(F32), by_a.astype(BF).astype(F32)
    scale = lax.rsqrt(jnp.mean(h**2, -1, keepdims=True) + 1e-6)
    return (by_a * scale - h * (scale**3 * jnp.mean(by_a * h, -1, keepdims=True))).astype(BF)


def last_body(width, n, h_ref, dy_ref, wg_ref, wu_ref, wd_ref, out_ref, ss_ref, by_ref, whole_ref, a_ref, at_ref, dyt_ref, da_ref, ws, wds, dgu, hid, *refs):
    c = pl.program_id(0)
    total = Sum(n, out_ref.shape[1], out_ref, ss_ref, refs, SPREAD, whole_ref)

    @pl.when(c == 0)
    def _():
        total.enter()
        da_ref[...] = jnp.zeros_like(da_ref)
        ss_ref[...] = jnp.zeros_like(ss_ref)
        a_ref[...] = normed(h_ref[...])
        turn(at_ref, lambda rows: a_ref[rows, :])
        turn(dyt_ref, lambda rows: dy_ref[rows, :])

    total.receive(c)

    @pl.when(c < n)
    def _():
        ws[:, :FC] = masked(c, width, 1, wg_ref[...])
        ws[:, FC:] = masked(c, width, 1, wu_ref[...])
        wds[...] = masked(c, width, 0, wd_ref[...])

        def tile(i, _):
            rows = pl.ds(pl.multiple_of(i * TM, TM), TM)
            gu = nn(a_ref[rows, :], ws[...])
            dh = nt(dy_ref[rows, :], wds[...]).astype(BF).astype(F32)
            h, dg, du = back(gu[:, :FC], gu[:, FC:], dh)
            hid[rows, :] = h
            dgu[rows, :FC] = dg
            dgu[rows, FC:] = du
            da_ref[rows, :] += nt(dgu[rows, :], ws[...])
            return 0

        lax.fori_loop(0, a_ref.shape[0] // TM, tile, 0, unroll=True)
        gradients(total, c, at_ref, dyt_ref, dgu, hid)

    total.send(c)

    @pl.when(c == n)
    def _():
        def tile(i, _):
            rows = pl.ds(pl.multiple_of(i * TM, TM), TM)
            by_ref[rows, :] = dy_ref[rows, :] + by_normed(h_ref[rows, :], da_ref[rows, :])
            return 0

        lax.fori_loop(0, by_ref.shape[0] // TM, tile, 0)


def last(layer, h, dy, w_gate, w_up, w_down):
    t, d = h.shape
    f = w_gate.shape[2]
    n = pl.cdiv(f, FC)
    rows = d // 8
    wcol = pl.BlockSpec((None, d, FC), lambda c: (layer, 0, jnp.minimum(c, n - 1)))
    wrow = pl.BlockSpec((None, FC, d), lambda c: (layer, jnp.minimum(c, n - 1), 0))
    return pl.pallas_call(
        functools.partial(last_body, f, n),
        grid=(n + 3 * LAG,),
        in_specs=[once((t, d)), once((t, d)), wcol, wcol, wrow],
        out_specs=[
            pl.BlockSpec((None, 3, rows, FC), lambda c: (jnp.maximum(c - 3 * LAG, 0), 0, 0, 0)),
            pl.BlockSpec((rows, FC), lambda c: (0, 0)),
            once((t, d)),
            pl.BlockSpec(memory_space=pl.ANY),
        ],
        out_shape=[
            jax.ShapeDtypeStruct((n, 3, rows, FC), BF),
            jax.ShapeDtypeStruct((rows, FC), F32),
            jax.ShapeDtypeStruct((t, d), BF),
            jax.ShapeDtypeStruct((8, SPREAD, 3, rows, FC), BF),
        ],
        scratch_shapes=[
            pltpu.VMEM((t, d), BF),
            pltpu.VMEM((d, t), BF),
            pltpu.VMEM((d, t), BF),
            pltpu.VMEM((t, d), F32),
            pltpu.VMEM((d, 2 * FC), BF),
            pltpu.VMEM((FC, d), BF),
            pltpu.VMEM((t, 2 * FC), BF),
            pltpu.VMEM((t, FC), BF),
            *Sum.scratch(rows),
            *Sum.spread_scratch(rows),
        ],
        compiler_params=params(collective_id=0, has_side_effects=True),
        cost_estimate=pl.CostEstimate(flops=16 * t * d * f, bytes_accessed=10 * d * f, transcendentals=t * f),
        name="last",
    )(h, dy, w_gate, w_up, w_down)


def first_body(width, n, x_ref, dy_ref, g_ref, u_ref, wd_ref, so_far_ref, out_ref, sum_ref, ss_ref, at_ref, dyt_ref, wds, dgu, hid, part, landed, part_sent, part_landed, *refs):
    c = pl.program_id(0)
    total = Sum(n, out_ref.shape[1], out_ref, ss_ref, refs)

    @pl.when(c == 0)
    def _():
        total.enter()
        ss_ref[...] = so_far_ref[...]
        turn(at_ref, lambda rows: normed(x_ref[rows, :]))
        turn(dyt_ref, lambda rows: dy_ref[rows, :])

    total.receive(c)

    @pl.when(c < n)
    def _():
        wds[...] = masked(c, width, 0, wd_ref[...])

        def tile(i, _):
            rows = pl.ds(pl.multiple_of(i * TM, TM), TM)
            dh = nt(dy_ref[rows, :], wds[...]).astype(BF).astype(F32)
            h, dg, du = back(g_ref[rows, :], u_ref[rows, :], dh)
            hid[rows, :] = h
            dgu[rows, :FC] = dg
            dgu[rows, FC:] = du
            return 0

        lax.fori_loop(0, dy_ref.shape[0] // TM, tile, 0, unroll=True)
        gradients(total, c, at_ref, dyt_ref, dgu, hid)

    total.send(c)

    @pl.when(c == n + 3 * LAG - 1)
    def _():
        part[0] = jnp.full(part.shape[1:], jnp.sum(ss_ref[...]))
        for stage in range(3):
            copy = pltpu.make_async_remote_copy(
                src_ref=part.at[stage],
                dst_ref=landed.at[stage],
                send_sem=part_sent.at[stage],
                recv_sem=part_landed.at[stage],
                device_id={"dp": total.over[stage]},
                device_id_type=pl.DeviceIdType.MESH,
            )
            copy.start()
            copy.wait()
            part[stage + 1] = part[stage] + landed[stage]
        sum_ref[...] = part[3]


def first(layer, x, dy, g, u, w_down, so_far):
    t, d = dy.shape
    f = w_down.shape[1]
    n = pl.cdiv(f, FC)
    rows = d // 8
    gu = pl.BlockSpec((t, FC), lambda c: (0, jnp.minimum(c, n - 1)))
    wrow = pl.BlockSpec((None, FC, d), lambda c: (layer, jnp.minimum(c, n - 1), 0))
    return pl.pallas_call(
        functools.partial(first_body, f, n),
        grid=(n + 3 * LAG,),
        in_specs=[once((t, d)), once((t, d)), gu, gu, wrow, once((rows, FC))],
        out_specs=[
            pl.BlockSpec((None, 3, rows, FC), lambda c: (jnp.maximum(c - 3 * LAG, 0), 0, 0, 0)),
            once((8, 128)),
        ],
        out_shape=[jax.ShapeDtypeStruct((n, 3, rows, FC), BF), jax.ShapeDtypeStruct((8, 128), F32)],
        scratch_shapes=[
            pltpu.VMEM((rows, FC), F32),
            pltpu.VMEM((d, t), BF),
            pltpu.VMEM((d, t), BF),
            pltpu.VMEM((FC, d), BF),
            pltpu.VMEM((t, 2 * FC), BF),
            pltpu.VMEM((t, FC), BF),
            pltpu.VMEM((4, 8, 128), F32),
            pltpu.VMEM((3, 8, 128), F32),
            pltpu.SemaphoreType.DMA((3,)),
            pltpu.SemaphoreType.DMA((3,)),
            *Sum.scratch(rows),
        ],
        compiler_params=params(collective_id=1, has_side_effects=True),
        cost_estimate=pl.CostEstimate(flops=8 * t * d * f, bytes_accessed=8 * t * f, transcendentals=t * f),
        name="first",
    )(x, dy, g, u, w_down, so_far)


def adamw_body(count, sum_ref, g_ref, *refs):
    ins, outs = refs[:9], refs[-9:]
    factor = jnp.minimum(1.0, 0.5 * lax.rsqrt(sum_ref[0:1, 0:1] / count + 1e-30))
    for i in range(3):
        w_ref, m_ref, v_ref = ins[i::3]
        w_out, m_out, v_out = outs[i::3]
        g = g_ref[:, i].reshape(-1, FC)
        g = (g.T if i == 2 else g).astype(F32) * factor
        m = 0.9 * m_ref[...] + 0.1 * g
        v = 0.95 * v_ref[...] + 0.05 * g * g
        w = w_ref[...].astype(F32)
        m_out[...] = m
        v_out[...] = v
        w_out[...] = (w - 0.02 * (m * lax.rsqrt(v + 1e-8) + 0.1 * w)).astype(BF)


def adamw(layer, start, squares, g, w, m, v, done):
    d, f = w[0].shape[1:]
    chunks = g.shape[1]
    wide = pl.BlockSpec((None, d, FC), lambda c: (layer, 0, c + start))
    tall = pl.BlockSpec((None, FC, d), lambda c: (layer, c + start, 0))
    blocks = [wide, wide, tall]
    gblock = pl.BlockSpec((8, None, 3, g.shape[3], FC), lambda c: (0, c, 0, 0, 0))
    size = 3 * d * FC * chunks
    return pl.pallas_call(
        functools.partial(adamw_body, sum(one.size for one in w)),
        grid=(chunks,),
        in_specs=[once((8, 128)), gblock, *blocks * 3] + [pl.BlockSpec(memory_space=pl.ANY)] * len(done),
        out_specs=blocks * 3,
        out_shape=[jax.ShapeDtypeStruct(o.shape, o.dtype) for o in (*w, *m, *v)],
        input_output_aliases={11 + i: i for i in range(len(done))},
        compiler_params=params(),
        cost_estimate=pl.CostEstimate(flops=120 * size, bytes_accessed=22 * size, transcendentals=size),
        name="adamw",
    )(squares, g, *w, *m, *v, *done)


def solution(mesh):
    def step(x, dy, *arrays):
        weights, m, v = (arrays[i : i + 3] for i in (0, 3, 6))
        x, dy = x[0], dy[0]
        gate, up, h = forward(0, x, *weights)
        shard1, so_far, by_h, early = last(1, h, dy, *weights)
        late = lax.all_gather(shard1[SPREAD:], "dp")
        shard0, squares = first(0, x, by_h, gate, up, weights[2], so_far)
        half = shard0.shape[0] // 2
        parts = [(1, 0, early), (1, SPREAD, late)]
        parts += [(0, start, lax.all_gather(part, "dp")) for start, part in ((0, shard0[:half]), (half, shard0[half:]))]
        new = ()
        for layer, start, part in parts:
            new = adamw(layer, start, squares, part, weights, m, v, new)
        return tuple(new)

    return jax.shard_map(
        step,
        mesh=mesh,
        in_specs=(P(("rep", "dp"), None, None),) * 2 + (P(None, None, None),) * 9,
        out_specs=(P("rep", None, None),) * 9,
        check_vma=False,
    )
```

```python
import functools

import jax
import jax.numpy as jnp
from jax import lax
from jax.experimental import pallas as pl
from jax.experimental.pallas import tpu as pltpu
from jax.sharding import PartitionSpec as P

BF, F32 = jnp.bfloat16, jnp.float32
FC = 256
TM = 512
LIMIT = 67_043_328
STARTS = (16, 28)
LAG = 2
SLOTS = 4


def normed(h):
    wide = h.astype(F32)
    scale = lax.rsqrt(jnp.mean(wide**2, -1, keepdims=True) + 1e-6)
    return (wide * scale).astype(BF)


def nt(a, b):
    return lax.dot_general(a, b, (((1,), (1,)), ((), ())), preferred_element_type=F32)


def nn(a, b):
    return jnp.dot(a, b, preferred_element_type=F32)


def masked(c, width, axis, w):
    place = lax.broadcasted_iota(jnp.int32, w.shape, axis) + c * FC
    return jnp.where(place < width, w, jnp.zeros_like(w))


def once(shape):
    return pl.BlockSpec(shape, lambda c: (0,) * len(shape), pipeline_mode=pl.Buffered(1))


def params(**more):
    return pltpu.CompilerParams(vmem_limit_bytes=LIMIT, dimension_semantics=("arbitrary",), **more)


def fwd_body(width, x_ref, wg_ref, wu_ref, wd_ref, g_ref, u_ref, h_ref, a_ref, acc, ws, wds):
    c = pl.program_id(0)

    @pl.when(c == 0)
    def _():
        acc[...] = jnp.zeros_like(acc)
        a_ref[...] = normed(x_ref[...])

    ws[:, :FC] = masked(c, width, 1, wg_ref[...])
    ws[:, FC:] = masked(c, width, 1, wu_ref[...])
    wds[...] = masked(c, width, 0, wd_ref[...])

    def tile(i, _):
        rows = pl.ds(pl.multiple_of(i * TM, TM), TM)
        gu = nn(a_ref[rows, :], ws[...])
        g, u = gu[:, :FC], gu[:, FC:]
        g_ref[rows, :] = g
        u_ref[rows, :] = u
        acc[rows, :] += nn((g * jax.nn.sigmoid(g) * u).astype(BF), wds[...])
        return 0

    lax.fori_loop(0, a_ref.shape[0] // TM, tile, 0, unroll=True)

    @pl.when(c == pl.num_programs(0) - 1)
    def _():
        h_ref[...] = x_ref[...] + acc[...].astype(BF)


def forward(layer, x, w_gate, w_up, w_down):
    t, d = x.shape
    f = w_gate.shape[2]
    n = pl.cdiv(f, FC)
    wcol = pl.BlockSpec((None, d, FC), lambda c: (layer, 0, c))
    wrow = pl.BlockSpec((None, FC, d), lambda c: (layer, c, 0))
    return pl.pallas_call(
        functools.partial(fwd_body, f),
        grid=(n,),
        in_specs=[once((t, d)), wcol, wcol, wrow],
        out_specs=[pl.BlockSpec((t, FC), lambda c: (0, c))] * 2 + [once((t, d))],
        out_shape=[jax.ShapeDtypeStruct((t, n * FC), F32)] * 2 + [jax.ShapeDtypeStruct((t, d), BF)],
        scratch_shapes=[pltpu.VMEM((t, d), BF), pltpu.VMEM((t, d), F32), pltpu.VMEM((d, 2 * FC), BF), pltpu.VMEM((FC, d), BF)],
        compiler_params=params(),
        cost_estimate=pl.CostEstimate(flops=6 * t * d * f, bytes_accessed=10 * t * f, transcendentals=t * f),
        name="forward",
    )(x, w_gate, w_up, w_down)


class Sum:
    def __init__(self, n, rows, out_refs, ss_ref, refs, spread, whole_ref):
        self.n, self.rows, self.outs, self.ss = n, rows, out_refs, ss_ref
        self.spread, self.whole = spread, whole_ref
        self.own, self.land0, self.send1, self.keep1, self.land1, self.send2, self.keep2, self.land2 = refs[:8]
        self.sends, self.lands = refs[8:14:2], refs[9:14:2]
        self.fin, self.local, *sems = refs[14:]
        self.out_sends, self.out_lands = sems[::2], sems[1::2]
        me = self.me = lax.axis_index("dp")
        self.x, self.y, self.core = me // 4, (me // 2) % 2, me % 2
        self.over = (me + 1 - 2 * self.core, me + 4 - 8 * self.x, me + 2 - 4 * self.y)

    @staticmethod
    def scratch(rows):
        def buffer(slots, *shape, dtype=BF):
            return pltpu.VMEM((slots, *shape, rows, FC), dtype)

        return [
            buffer(2, 2, 3, 4),
            buffer(SLOTS, 3, 4),
            buffer(2, 3, 2),
            buffer(2, 3, 2, dtype=F32),
            buffer(SLOTS, 3, 2),
            buffer(2, 3),
            buffer(2, 3, dtype=F32),
            buffer(SLOTS, 3),
        ] + [pltpu.SemaphoreType.DMA((2,)), pltpu.SemaphoreType.DMA((SLOTS,))] * 3

    @staticmethod
    def spread_scratch(rows):
        sems = [pltpu.SemaphoreType.DMA((slots, copies)) for copies in (1, 2, 4) for slots in (2, SLOTS)]
        return [pltpu.VMEM((2, 3, rows, FC), BF), pltpu.SemaphoreType.DMA((2,)), *sems]

    def enter(self):
        barrier = pltpu.get_barrier_semaphore()
        for other in self.over:
            pl.semaphore_signal(barrier, inc=1, device_id={"dp": other}, device_id_type=pl.DeviceIdType.MESH)
        pl.semaphore_wait(barrier, 3)

    def put(self, c, which, g):
        slot = lax.rem(c, 2)
        for j in range(8):
            core, x, y = (j % 2 + self.core) % 2, (j // 4 + self.x) % 2, ((j // 2) % 2 + self.y) % 2
            self.own[slot, core, which, x * 2 + y] = g[j * self.rows : (j + 1) * self.rows].astype(BF)

    def copy(self, stage, k):
        two, four, odd = lax.rem(k, 2), lax.rem(k, SLOTS), lax.rem(k, 2)
        if stage == 0:
            src, dst, to = self.own.at[two, 1], self.land0.at[four], self.over[0]
        elif stage == 1:
            src, dst, to = self.send1.at[two], self.land1.at[four], self.over[1] * (1 - odd) + self.over[2] * odd
        else:
            src, dst, to = self.send2.at[two], self.land2.at[four], self.over[2] * (1 - odd) + self.over[1] * odd
        return pltpu.make_async_remote_copy(
            src_ref=src,
            dst_ref=dst,
            send_sem=self.sends[stage].at[two],
            recv_sem=self.lands[stage].at[four],
            device_id={"dp": to},
            device_id_type=pl.DeviceIdType.MESH,
        )

    def when(self, k, n=None):
        return pl.when((k >= 0) & (k < (self.n if n is None else n)))

    def keep(self, k):
        return pltpu.make_async_copy(self.fin.at[lax.rem(k, 2)], self.whole.at[self.me, k], self.local.at[lax.rem(k, 2)])

    def give(self, stage, k):
        two, four, odd = lax.rem(k, 2), lax.rem(k, SLOTS), lax.rem(k, 2)
        near = self.over[1] * (1 - odd) + self.over[2] * odd
        far = self.over[2] * (1 - odd) + self.over[1] * odd
        blocks = (self.me, far, near, near + far - self.me)[: 2**stage]
        to = (far, near, self.over[0])[stage]
        return [
            pltpu.make_async_remote_copy(
                src_ref=self.whole.at[block, k] if stage else self.fin.at[two],
                dst_ref=self.whole.at[block, k],
                send_sem=self.out_sends[stage].at[two, i],
                recv_sem=self.out_lands[stage].at[four, i],
                device_id={"dp": to},
                device_id_type=pl.DeviceIdType.MESH,
            )
            for i, block in enumerate(blocks)
        ]

    def receive(self, c):
        for stage in (2, 1, 0):
            k = c - (4 + stage) * LAG

            @self.when(k, self.spread)
            def _(stage=stage, k=k):
                if stage == 0:
                    self.keep(k).wait()
                for copy in self.give(stage, k):
                    copy.wait()

        k2 = c - 3 * LAG

        @self.when(k2)
        def _():
            self.copy(2, k2).wait()
            g = (self.keep2[lax.rem(k2, 2)] + self.land2[lax.rem(k2, SLOTS)].astype(F32)).astype(BF)
            self.fin[lax.rem(k2, 2)] = g
            for start, end, out_ref in self.outs:

                @pl.when((k2 >= start) & (k2 < end))
                def _(out_ref=out_ref):
                    out_ref[...] = g

            g = g.astype(F32)
            self.ss[...] += g[0] * g[0] + g[1] * g[1] + g[2] * g[2]

        k1 = c - 2 * LAG

        @self.when(k1)
        def _():
            self.copy(1, k1).wait()
            two, four = lax.rem(k1, 2), lax.rem(k1, SLOTS)
            self.keep2[two] = self.keep1[two, :, 0] + self.land1[four, :, 0].astype(F32)
            self.send2[two] = (self.keep1[two, :, 1] + self.land1[four, :, 1].astype(F32)).astype(BF)

        k0 = c - LAG

        @self.when(k0)
        def _():
            self.copy(0, k0).wait()
            two, four = lax.rem(k0, 2), lax.rem(k0, SLOTS)
            odd = two
            for to, place in ((0, 0), (1, 1 + odd)):
                self.keep1[two, :, to] = self.own[two, 0, :, place].astype(F32) + self.land0[four, :, place].astype(F32)
            for to, place in ((0, 2 - odd), (1, 3)):
                self.send1[two, :, to] = (self.own[two, 0, :, place].astype(F32) + self.land0[four, :, place].astype(F32)).astype(BF)

    def send_own(self, c):
        @self.when(c)
        def _():
            self.copy(0, c).start()

    def send(self, c):
        for stage in (1, 2):
            k = c - stage * LAG

            @self.when(k)
            def _(stage=stage, k=k):
                self.copy(stage, k).start()

        for stage in range(3):
            k = c - (3 + stage) * LAG

            @self.when(k, self.spread)
            def _(stage=stage, k=k):
                if stage == 0:
                    self.keep(k).start()
                for copy in self.give(stage, k):
                    copy.start()


def back(g, u, dh):
    s = jax.nn.sigmoid(g)
    silu = g * s
    return (silu * u).astype(BF), (dh * u * (s + silu * (1 - s))).astype(BF), (dh * silu).astype(BF)


def gradients(total, c, at_ref, dyt_ref, dgu, hid):
    o = nn(at_ref[...], dgu[...])
    total.put(c, 0, o[:, :FC])
    total.put(c, 1, o[:, FC:])
    total.put(c, 2, nn(dyt_ref[...], hid[...]))


def turn(to_ref, of):
    for i in range(to_ref.shape[1] // TM):
        rows = pl.ds(i * TM, TM)
        to_ref[:, rows] = of(rows).T


def by_normed(h, by_a):
    h, by_a = h.astype(F32), by_a.astype(BF).astype(F32)
    scale = lax.rsqrt(jnp.mean(h**2, -1, keepdims=True) + 1e-6)
    return (by_a * scale - h * (scale**3 * jnp.mean(by_a * h, -1, keepdims=True))).astype(BF)


def middle_body(
    width, n, starts, h_ref, x_ref, dy_ref, wg_ref, wu_ref, wd_ref, g_ref, u_ref, whole_ref, out1_ref, out2_ref, sum_ref,
    ss, hx, a, at, dyt, da, ws, wds, dgu, hid, part, landed, part_sent, part_landed, load, *refs,
):
    c = pl.program_id(0)
    total = Sum(2 * n, out1_ref.shape[1], tuple(zip(starts, (starts[1], 2 * n), (out1_ref, out2_ref), strict=True)), ss, refs, starts[0], whole_ref)
    tiles = dy_ref.shape[0] // TM

    def fetch(ref):
        copy = pltpu.make_async_copy(ref, hx, load)
        copy.start()
        copy.wait()

    @pl.when(c == 0)
    def _():
        total.enter()
        fetch(h_ref)
        da[...] = jnp.zeros_like(da)
        ss[...] = jnp.zeros_like(ss)
        a[...] = normed(hx[...])
        turn(at, lambda rows: a[rows, :])
        turn(dyt, lambda rows: dy_ref[rows, :])

    total.receive(c)
    total.send(c)

    @pl.when(c < n)
    def _():
        ws[:, :FC] = masked(c, width, 1, wg_ref[...])
        ws[:, FC:] = masked(c, width, 1, wu_ref[...])
        wds[...] = masked(c, width, 0, wd_ref[...])

        def heads(rows):
            return nn(a[rows, :], ws[...]), nt(dy_ref[rows, :], wds[...])

        def tail(rows):
            da[rows, :] += nt(dgu[rows, :], ws[...])

        places = [slice(i * TM, (i + 1) * TM) for i in range(tiles)]
        ahead = heads(places[0])
        for i, rows in enumerate(places):
            gu, dh = ahead
            if i + 1 < tiles:
                ahead = heads(places[i + 1])
            h, dg, du = back(gu[:, :FC], gu[:, FC:], dh.astype(BF).astype(F32))
            hid[rows, :] = h
            dgu[rows, :FC] = dg
            dgu[rows, FC:] = du
            if i:
                tail(places[i - 1])
        tail(places[-1])
        gradients(total, c, at, dyt, dgu, hid)

    @pl.when(c == n)
    def _():
        def tile(i, _):
            rows = pl.ds(pl.multiple_of(i * TM, TM), TM)
            a[rows, :] = dy_ref[rows, :] + by_normed(hx[rows, :], da[rows, :])
            return 0

        lax.fori_loop(0, tiles, tile, 0)
        fetch(x_ref)
        turn(at, lambda rows: normed(hx[rows, :]))
        turn(dyt, lambda rows: a[rows, :])

    @pl.when((c >= n) & (c < 2 * n))
    def _():
        wds[...] = masked(c - n, width, 0, wd_ref[...])

        def tile(i, _):
            rows = pl.ds(pl.multiple_of(i * TM, TM), TM)
            dh = nt(a[rows, :], wds[...]).astype(BF).astype(F32)
            h, dg, du = back(g_ref[rows, :], u_ref[rows, :], dh)
            hid[rows, :] = h
            dgu[rows, :FC] = dg
            dgu[rows, FC:] = du
            return 0

        lax.fori_loop(0, tiles, tile, 0, unroll=True)
        gradients(total, c, at, dyt, dgu, hid)

    total.send_own(c)

    @pl.when(c == 2 * n + 3 * LAG - 1)
    def _():
        part[0] = jnp.full(part.shape[1:], jnp.sum(ss[...]))
        for stage in range(3):
            copy = pltpu.make_async_remote_copy(
                src_ref=part.at[stage],
                dst_ref=landed.at[stage],
                send_sem=part_sent.at[stage],
                recv_sem=part_landed.at[stage],
                device_id={"dp": total.over[stage]},
                device_id_type=pl.DeviceIdType.MESH,
            )
            copy.start()
            copy.wait()
            part[stage + 1] = part[stage] + landed[stage]
        sum_ref[...] = part[3]


def middle(h, x, dy, g, u, w_gate, w_up, w_down, starts):
    t, d = h.shape
    f = w_gate.shape[2]
    n = pl.cdiv(f, FC)
    rows = d // 8
    wcol = pl.BlockSpec((None, d, FC), lambda c: (1, 0, jnp.minimum(c, n - 1)))
    wrow = pl.BlockSpec((None, FC, d), lambda c: (1 - jnp.minimum(c // n, 1), jnp.minimum(c - n * jnp.minimum(c // n, 1), n - 1), 0))
    gu = pl.BlockSpec((t, FC), lambda c: (0, jnp.clip(c - n, 0, n - 1)))
    sizes = starts[1] - starts[0], 2 * n - starts[1]
    outs = [
        pl.BlockSpec((None, 3, rows, FC), lambda c, i=i: (jnp.clip(c - 3 * LAG - starts[i], 0, sizes[i] - 1), 0, 0, 0)) for i in range(2)
    ]
    anywhere = pl.BlockSpec(memory_space=pl.ANY)
    return pl.pallas_call(
        functools.partial(middle_body, f, n, starts),
        grid=(2 * n + 3 * LAG,),
        in_specs=[anywhere, anywhere, once((t, d)), wcol, wcol, wrow, gu, gu],
        out_specs=[anywhere, *outs, once((8, 128))],
        out_shape=[
            jax.ShapeDtypeStruct((8, starts[0], 3, rows, FC), BF),
            *(jax.ShapeDtypeStruct((size, 3, rows, FC), BF) for size in sizes),
            jax.ShapeDtypeStruct((8, 128), F32),
        ],
        scratch_shapes=[
            pltpu.VMEM((rows, FC), F32),
            pltpu.VMEM((t, d), BF),
            pltpu.VMEM((t, d), BF),
            pltpu.VMEM((d, t), BF),
            pltpu.VMEM((d, t), BF),
            pltpu.VMEM((t, d), F32),
            pltpu.VMEM((d, 2 * FC), BF),
            pltpu.VMEM((FC, d), BF),
            pltpu.VMEM((t, 2 * FC), BF),
            pltpu.VMEM((t, FC), BF),
            pltpu.VMEM((4, 8, 128), F32),
            pltpu.VMEM((3, 8, 128), F32),
            pltpu.SemaphoreType.DMA((3,)),
            pltpu.SemaphoreType.DMA((3,)),
            pltpu.SemaphoreType.DMA,
            *Sum.scratch(rows),
            *Sum.spread_scratch(rows),
        ],
        compiler_params=params(collective_id=0, has_side_effects=True),
        cost_estimate=pl.CostEstimate(flops=24 * t * d * f, bytes_accessed=8 * t * f, transcendentals=2 * t * f),
        name="middle",
    )(h, x, dy, w_gate, w_up, w_down, g, u)


def adamw_body(count, sum_ref, g_ref, *refs):
    ins, outs = refs[:9], refs[-9:]
    factor = jnp.minimum(1.0, 0.5 * lax.rsqrt(sum_ref[0:1, 0:1] / count + 1e-30))

    def update(i, g, place):
        w_ref, m_ref, v_ref = ins[i::3]
        w_out, m_out, v_out = outs[i::3]
        g = g.astype(F32) * factor
        m = 0.9 * m_ref[place] + 0.1 * g
        v = 0.95 * v_ref[place] + 0.05 * g * g
        w = w_ref[place].astype(F32)
        m_out[place] = m
        v_out[place] = v
        w_out[place] = (w - 0.02 * (m * lax.rsqrt(v + 1e-8) + 0.1 * w)).astype(BF)

    rows = g_ref.shape[2]

    def block(j, _):
        for i in range(2):
            update(i, g_ref[j, i], (pl.ds(pl.multiple_of(j * rows, rows), rows), slice(None)))
        return 0

    lax.fori_loop(0, 8, block, 0)
    for j in range(0, FC, 128):
        update(2, g_ref[:, 2, :, j : j + 128].reshape(-1, 128).T, (slice(j, j + 128), slice(None)))


def adamw(start, squares, g, w, m, v, done):
    d, f = w[0].shape[1:]
    n, chunks = pl.cdiv(f, FC), g.shape[1]
    wide = pl.BlockSpec((None, d, FC), lambda c: (1 - (c + start) // n, 0, lax.rem(c + start, n)))
    tall = pl.BlockSpec((None, FC, d), lambda c: (1 - (c + start) // n, lax.rem(c + start, n), 0))
    blocks = [wide, wide, tall]
    gblock = pl.BlockSpec((8, None, 3, g.shape[3], FC), lambda c: (0, c, 0, 0, 0))
    size = 3 * d * FC * chunks
    return pl.pallas_call(
        functools.partial(adamw_body, sum(one.size for one in w)),
        grid=(chunks,),
        in_specs=[once((8, 128)), gblock, *blocks * 3] + [pl.BlockSpec(memory_space=pl.ANY)] * len(done),
        out_specs=blocks * 3,
        out_shape=[jax.ShapeDtypeStruct(o.shape, o.dtype) for o in (*w, *m, *v)],
        input_output_aliases={11 + i: i for i in range(len(done))},
        compiler_params=params(),
        cost_estimate=pl.CostEstimate(flops=120 * size, bytes_accessed=22 * size, transcendentals=size),
        name="adamw",
    )(squares, g, *w, *m, *v, *done)


def solution(mesh):
    def step(x, dy, *arrays):
        weights, m, v = (arrays[i : i + 3] for i in (0, 3, 6))
        x, dy = x[0], dy[0]
        gate, up, h = forward(0, x, *weights)
        whole, one, two, squares = middle(h, x, dy, gate, up, *weights, STARTS)
        parts = [(0, whole), (STARTS[0], lax.all_gather(one, "dp")), (STARTS[1], lax.all_gather(two, "dp"))]
        new = ()
        for start, part in parts:
            new = adamw(start, squares, part, weights, m, v, new)
        return tuple(new)

    return jax.shard_map(
        step,
        mesh=mesh,
        in_specs=(P(("rep", "dp"), None, None),) * 2 + (P(None, None, None),) * 9,
        out_specs=(P("rep", None, None),) * 9,
        check_vma=False,
    )
```

```python
import functools

import jax
import jax.numpy as jnp
from jax import lax
from jax.experimental import pallas as pl
from jax.experimental.pallas import tpu as pltpu
from jax.sharding import PartitionSpec as P

BF, F32 = jnp.bfloat16, jnp.float32
FC = 256
TM = 512
LIMIT = 67_043_328
STARTS = (16, 29)
LAG = 2
SLOTS = 4


def normed(h):
    wide = h.astype(F32)
    scale = lax.rsqrt(jnp.mean(wide**2, -1, keepdims=True) + 1e-6)
    return (wide * scale).astype(BF)


def nt(a, b):
    return lax.dot_general(a, b, (((1,), (1,)), ((), ())), preferred_element_type=F32)


def nn(a, b):
    return jnp.dot(a, b, preferred_element_type=F32)


def masked(c, width, axis, w):
    place = lax.broadcasted_iota(jnp.int32, w.shape, axis) + c * FC
    return jnp.where(place < width, w, jnp.zeros_like(w))


def once(shape):
    return pl.BlockSpec(shape, lambda c: (0,) * len(shape), pipeline_mode=pl.Buffered(1))


def params(**more):
    return pltpu.CompilerParams(vmem_limit_bytes=LIMIT, dimension_semantics=("arbitrary",), **more)


def fwd_body(width, x_ref, wg_ref, wu_ref, wd_ref, g_ref, u_ref, h_ref, a_ref, acc, ws, wds):
    c = pl.program_id(0)

    @pl.when(c == 0)
    def _():
        acc[...] = jnp.zeros_like(acc)
        a_ref[...] = normed(x_ref[...])

    ws[:, :FC] = masked(c, width, 1, wg_ref[...])
    ws[:, FC:] = masked(c, width, 1, wu_ref[...])
    wds[...] = masked(c, width, 0, wd_ref[...])

    def tile(i, _):
        rows = pl.ds(pl.multiple_of(i * TM, TM), TM)
        gu = nn(a_ref[rows, :], ws[...])
        g, u = gu[:, :FC], gu[:, FC:]
        g_ref[rows, :] = g
        u_ref[rows, :] = u
        acc[rows, :] += nn((g * jax.nn.sigmoid(g) * u).astype(BF), wds[...])
        return 0

    lax.fori_loop(0, a_ref.shape[0] // TM, tile, 0, unroll=True)

    @pl.when(c == pl.num_programs(0) - 1)
    def _():
        h_ref[...] = x_ref[...] + acc[...].astype(BF)


def forward(layer, x, w_gate, w_up, w_down):
    t, d = x.shape
    f = w_gate.shape[2]
    n = pl.cdiv(f, FC)
    wcol = pl.BlockSpec((None, d, FC), lambda c: (layer, 0, c))
    wrow = pl.BlockSpec((None, FC, d), lambda c: (layer, c, 0))
    return pl.pallas_call(
        functools.partial(fwd_body, f),
        grid=(n,),
        in_specs=[once((t, d)), wcol, wcol, wrow],
        out_specs=[pl.BlockSpec((t, FC), lambda c: (0, c))] * 2 + [once((t, d))],
        out_shape=[jax.ShapeDtypeStruct((t, n * FC), F32)] * 2 + [jax.ShapeDtypeStruct((t, d), BF)],
        scratch_shapes=[pltpu.VMEM((t, d), BF), pltpu.VMEM((t, d), F32), pltpu.VMEM((d, 2 * FC), BF), pltpu.VMEM((FC, d), BF)],
        compiler_params=params(),
        cost_estimate=pl.CostEstimate(flops=6 * t * d * f, bytes_accessed=10 * t * f, transcendentals=t * f),
        name="forward",
    )(x, w_gate, w_up, w_down)


class Sum:
    def __init__(self, n, rows, out_refs, ss_ref, refs, spread, whole_ref):
        self.n, self.rows, self.outs, self.ss = n, rows, out_refs, ss_ref
        self.spread, self.whole = spread, whole_ref
        self.own, self.land0, self.send1, self.keep1, self.land1, self.send2, self.keep2, self.land2 = refs[:8]
        self.sends, self.lands = refs[8:14:2], refs[9:14:2]
        self.fin, self.local, *sems = refs[14:]
        self.out_sends, self.out_lands = sems[::2], sems[1::2]
        me = self.me = lax.axis_index("dp")
        self.x, self.y, self.core = me // 4, (me // 2) % 2, me % 2
        self.over = (me + 1 - 2 * self.core, me + 4 - 8 * self.x, me + 2 - 4 * self.y)

    @staticmethod
    def scratch(rows):
        def buffer(slots, *shape, dtype=BF):
            return pltpu.VMEM((slots, *shape, rows, FC), dtype)

        return [
            buffer(2, 2, 3, 4),
            buffer(SLOTS, 3, 4),
            buffer(2, 3, 2),
            buffer(2, 3, 2, dtype=F32),
            buffer(SLOTS, 3, 2),
            buffer(2, 3),
            buffer(2, 3, dtype=F32),
            buffer(SLOTS, 3),
        ] + [pltpu.SemaphoreType.DMA((2,)), pltpu.SemaphoreType.DMA((SLOTS,))] * 3

    @staticmethod
    def spread_scratch(rows):
        sems = [pltpu.SemaphoreType.DMA((slots, copies)) for copies in (1, 2, 4) for slots in (2, SLOTS)]
        return [pltpu.VMEM((2, 3, rows, FC), BF), pltpu.SemaphoreType.DMA((2,)), *sems]

    def enter(self):
        barrier = pltpu.get_barrier_semaphore()
        for other in self.over:
            pl.semaphore_signal(barrier, inc=1, device_id={"dp": other}, device_id_type=pl.DeviceIdType.MESH)
        pl.semaphore_wait(barrier, 3)

    def put(self, c, which, g):
        slot = lax.rem(c, 2)
        for j in range(8):
            core, x, y = (j % 2 + self.core) % 2, (j // 4 + self.x) % 2, ((j // 2) % 2 + self.y) % 2
            self.own[slot, core, which, x * 2 + y] = g[j * self.rows : (j + 1) * self.rows].astype(BF)

    def copy(self, stage, k):
        two, four, odd = lax.rem(k, 2), lax.rem(k, SLOTS), lax.rem(k, 2)
        if stage == 0:
            src, dst, to = self.own.at[two, 1], self.land0.at[four], self.over[0]
        elif stage == 1:
            src, dst, to = self.send1.at[two], self.land1.at[four], self.over[1] * (1 - odd) + self.over[2] * odd
        else:
            src, dst, to = self.send2.at[two], self.land2.at[four], self.over[2] * (1 - odd) + self.over[1] * odd
        return pltpu.make_async_remote_copy(
            src_ref=src,
            dst_ref=dst,
            send_sem=self.sends[stage].at[two],
            recv_sem=self.lands[stage].at[four],
            device_id={"dp": to},
            device_id_type=pl.DeviceIdType.MESH,
        )

    def when(self, k, n=None):
        return pl.when((k >= 0) & (k < (self.n if n is None else n)))

    def keep(self, k):
        return pltpu.make_async_copy(self.fin.at[lax.rem(k, 2)], self.whole.at[self.me, k], self.local.at[lax.rem(k, 2)])

    def give(self, stage, k):
        two, four, odd = lax.rem(k, 2), lax.rem(k, SLOTS), lax.rem(k, 2)
        near = self.over[1] * (1 - odd) + self.over[2] * odd
        far = self.over[2] * (1 - odd) + self.over[1] * odd
        blocks = (self.me, far, near, near + far - self.me)[: 2**stage]
        to = (far, near, self.over[0])[stage]
        return [
            pltpu.make_async_remote_copy(
                src_ref=self.whole.at[block, k] if stage else self.fin.at[two],
                dst_ref=self.whole.at[block, k],
                send_sem=self.out_sends[stage].at[two, i],
                recv_sem=self.out_lands[stage].at[four, i],
                device_id={"dp": to},
                device_id_type=pl.DeviceIdType.MESH,
            )
            for i, block in enumerate(blocks)
        ]

    def receive(self, c):
        for stage in (2, 1, 0):
            k = c - (4 + stage) * LAG

            @self.when(k, self.spread)
            def _(stage=stage, k=k):
                if stage == 0:
                    self.keep(k).wait()
                for copy in self.give(stage, k):
                    copy.wait()

        k2 = c - 3 * LAG

        @self.when(k2)
        def _():
            self.copy(2, k2).wait()
            g = (self.keep2[lax.rem(k2, 2)] + self.land2[lax.rem(k2, SLOTS)].astype(F32)).astype(BF)
            self.fin[lax.rem(k2, 2)] = g
            for start, end, out_ref in self.outs:

                @pl.when((k2 >= start) & (k2 < end))
                def _(out_ref=out_ref):
                    out_ref[...] = g

            g = g.astype(F32)
            self.ss[...] += g[0] * g[0] + g[1] * g[1] + g[2] * g[2]

        k1 = c - 2 * LAG

        @self.when(k1)
        def _():
            self.copy(1, k1).wait()
            two, four = lax.rem(k1, 2), lax.rem(k1, SLOTS)
            self.keep2[two] = self.keep1[two, :, 0] + self.land1[four, :, 0].astype(F32)
            self.send2[two] = (self.keep1[two, :, 1] + self.land1[four, :, 1].astype(F32)).astype(BF)

        k0 = c - LAG

        @self.when(k0)
        def _():
            self.copy(0, k0).wait()
            two, four = lax.rem(k0, 2), lax.rem(k0, SLOTS)
            odd = two
            for to, place in ((0, 0), (1, 1 + odd)):
                self.keep1[two, :, to] = self.own[two, 0, :, place].astype(F32) + self.land0[four, :, place].astype(F32)
            for to, place in ((0, 2 - odd), (1, 3)):
                self.send1[two, :, to] = (self.own[two, 0, :, place].astype(F32) + self.land0[four, :, place].astype(F32)).astype(BF)

    def send_own(self, c):
        @self.when(c)
        def _():
            self.copy(0, c).start()

    def send(self, c):
        for stage in (1, 2):
            k = c - stage * LAG

            @self.when(k)
            def _(stage=stage, k=k):
                self.copy(stage, k).start()

        for stage in range(3):
            k = c - (3 + stage) * LAG

            @self.when(k, self.spread)
            def _(stage=stage, k=k):
                if stage == 0:
                    self.keep(k).start()
                for copy in self.give(stage, k):
                    copy.start()


def back(g, u, dh):
    s = jax.nn.sigmoid(g)
    silu = g * s
    return (silu * u).astype(BF), (dh * u * (s + silu * (1 - s))).astype(BF), (dh * silu).astype(BF)


def gradients(total, c, at_ref, dyt_ref, dgu, hid):
    o = nn(at_ref[...], dgu[...])
    total.put(c, 0, o[:, :FC])
    total.put(c, 1, o[:, FC:])
    total.put(c, 2, nn(dyt_ref[...], hid[...]))


def turn(to_ref, of):
    for i in range(to_ref.shape[1] // TM):
        rows = pl.ds(i * TM, TM)
        to_ref[:, rows] = of(rows).T


def by_normed(h, by_a):
    h, by_a = h.astype(F32), by_a.astype(BF).astype(F32)
    scale = lax.rsqrt(jnp.mean(h**2, -1, keepdims=True) + 1e-6)
    return (by_a * scale - h * (scale**3 * jnp.mean(by_a * h, -1, keepdims=True))).astype(BF)


def middle_body(
    width, n, starts, h_ref, x_ref, dy_ref, wg_ref, wu_ref, wd_ref, g_ref, u_ref, whole_ref, out1_ref, out2_ref, sum_ref,
    ss, hx, a, at, dyt, da, ws, wds, dgu, hid, part, landed, part_sent, part_landed, load, *refs,
):
    c = pl.program_id(0)
    total = Sum(2 * n, out1_ref.shape[1], tuple(zip(starts, (starts[1], 2 * n), (out1_ref, out2_ref), strict=True)), ss, refs, starts[0], whole_ref)
    tiles = dy_ref.shape[0] // TM

    def fetch(ref):
        copy = pltpu.make_async_copy(ref, hx, load)
        copy.start()
        copy.wait()

    @pl.when(c == 0)
    def _():
        total.enter()
        fetch(h_ref)
        da[...] = jnp.zeros_like(da)
        ss[...] = jnp.zeros_like(ss)
        a[...] = normed(hx[...])
        turn(at, lambda rows: a[rows, :])
        turn(dyt, lambda rows: dy_ref[rows, :])

    total.receive(c)
    total.send(c)

    @pl.when(c < n)
    def _():
        ws[:, :FC] = masked(c, width, 1, wg_ref[...])
        ws[:, FC:] = masked(c, width, 1, wu_ref[...])
        wds[...] = masked(c, width, 0, wd_ref[...])

        def heads(rows):
            return nn(a[rows, :], ws[...]), nt(dy_ref[rows, :], wds[...])

        def tail(rows):
            da[rows, :] += nt(dgu[rows, :], ws[...])

        places = [slice(i * TM, (i + 1) * TM) for i in range(tiles)]
        ahead = heads(places[0])
        for i, rows in enumerate(places):
            gu, dh = ahead
            if i + 1 < tiles:
                ahead = heads(places[i + 1])
            h, dg, du = back(gu[:, :FC], gu[:, FC:], dh.astype(BF).astype(F32))
            hid[rows, :] = h
            dgu[rows, :FC] = dg
            dgu[rows, FC:] = du
            if i:
                tail(places[i - 1])
        tail(places[-1])
        gradients(total, c, at, dyt, dgu, hid)

    @pl.when(c == n)
    def _():
        def tile(i, _):
            rows = pl.ds(pl.multiple_of(i * TM, TM), TM)
            a[rows, :] = dy_ref[rows, :] + by_normed(hx[rows, :], da[rows, :])
            return 0

        lax.fori_loop(0, tiles, tile, 0)
        fetch(x_ref)
        turn(at, lambda rows: normed(hx[rows, :]))
        turn(dyt, lambda rows: a[rows, :])

    @pl.when((c >= n) & (c < 2 * n))
    def _():
        wds[...] = masked(c - n, width, 0, wd_ref[...])

        def tile(i, _):
            rows = pl.ds(pl.multiple_of(i * TM, TM), TM)
            dh = nt(a[rows, :], wds[...]).astype(BF).astype(F32)
            h, dg, du = back(g_ref[rows, :], u_ref[rows, :], dh)
            hid[rows, :] = h
            dgu[rows, :FC] = dg
            dgu[rows, FC:] = du
            return 0

        lax.fori_loop(0, tiles, tile, 0, unroll=True)
        gradients(total, c, at, dyt, dgu, hid)

    total.send_own(c)

    @pl.when(c == 2 * n + 3 * LAG - 1)
    def _():
        part[0] = jnp.full(part.shape[1:], jnp.sum(ss[...]))
        for stage in range(3):
            copy = pltpu.make_async_remote_copy(
                src_ref=part.at[stage],
                dst_ref=landed.at[stage],
                send_sem=part_sent.at[stage],
                recv_sem=part_landed.at[stage],
                device_id={"dp": total.over[stage]},
                device_id_type=pl.DeviceIdType.MESH,
            )
            copy.start()
            copy.wait()
            part[stage + 1] = part[stage] + landed[stage]
        sum_ref[...] = part[3]


def middle(h, x, dy, g, u, w_gate, w_up, w_down, starts):
    t, d = h.shape
    f = w_gate.shape[2]
    n = pl.cdiv(f, FC)
    rows = d // 8
    wcol = pl.BlockSpec((None, d, FC), lambda c: (1, 0, jnp.minimum(c, n - 1)))
    wrow = pl.BlockSpec((None, FC, d), lambda c: (1 - jnp.minimum(c // n, 1), jnp.minimum(c - n * jnp.minimum(c // n, 1), n - 1), 0))
    gu = pl.BlockSpec((t, FC), lambda c: (0, jnp.clip(c - n, 0, n - 1)))
    sizes = starts[1] - starts[0], 2 * n - starts[1]
    outs = [
        pl.BlockSpec((None, 3, rows, FC), lambda c, i=i: (jnp.clip(c - 3 * LAG - starts[i], 0, sizes[i] - 1), 0, 0, 0)) for i in range(2)
    ]
    anywhere = pl.BlockSpec(memory_space=pl.ANY)
    return pl.pallas_call(
        functools.partial(middle_body, f, n, starts),
        grid=(2 * n + 3 * LAG,),
        in_specs=[anywhere, anywhere, once((t, d)), wcol, wcol, wrow, gu, gu],
        out_specs=[anywhere, *outs, once((8, 128))],
        out_shape=[
            jax.ShapeDtypeStruct((8, starts[0], 3, rows, FC), BF),
            *(jax.ShapeDtypeStruct((size, 3, rows, FC), BF) for size in sizes),
            jax.ShapeDtypeStruct((8, 128), F32),
        ],
        scratch_shapes=[
            pltpu.VMEM((rows, FC), F32),
            pltpu.VMEM((t, d), BF),
            pltpu.VMEM((t, d), BF),
            pltpu.VMEM((d, t), BF),
            pltpu.VMEM((d, t), BF),
            pltpu.VMEM((t, d), F32),
            pltpu.VMEM((d, 2 * FC), BF),
            pltpu.VMEM((FC, d), BF),
            pltpu.VMEM((t, 2 * FC), BF),
            pltpu.VMEM((t, FC), BF),
            pltpu.VMEM((4, 8, 128), F32),
            pltpu.VMEM((3, 8, 128), F32),
            pltpu.SemaphoreType.DMA((3,)),
            pltpu.SemaphoreType.DMA((3,)),
            pltpu.SemaphoreType.DMA,
            *Sum.scratch(rows),
            *Sum.spread_scratch(rows),
        ],
        compiler_params=params(collective_id=0, has_side_effects=True),
        cost_estimate=pl.CostEstimate(flops=24 * t * d * f, bytes_accessed=8 * t * f, transcendentals=2 * t * f),
        name="middle",
    )(h, x, dy, w_gate, w_up, w_down, g, u)


def adamw_body(count, sum_ref, g_ref, *refs):
    ins, outs = refs[:9], refs[-9:]
    factor = jnp.minimum(1.0, 0.5 * lax.rsqrt(sum_ref[0:1, 0:1] / count + 1e-30))

    def update(i, g, place):
        w_ref, m_ref, v_ref = ins[i::3]
        w_out, m_out, v_out = outs[i::3]
        g = g.astype(F32) * factor
        m = 0.9 * m_ref[place] + 0.1 * g
        v = 0.95 * v_ref[place] + 0.05 * g * g
        w = w_ref[place].astype(F32)
        m_out[place] = m
        v_out[place] = v
        w_out[place] = (w - 0.02 * (m * lax.rsqrt(v + 1e-8) + 0.1 * w)).astype(BF)

    rows = g_ref.shape[2]

    def block(j, _):
        for i in range(2):
            update(i, g_ref[j, i], (pl.ds(pl.multiple_of(j * rows, rows), rows), slice(None)))
        return 0

    lax.fori_loop(0, 8, block, 0)
    for j in range(0, FC, 128):
        update(2, g_ref[:, 2, :, j : j + 128].reshape(-1, 128).T, (slice(j, j + 128), slice(None)))


def adamw(start, squares, g, w, m, v, done):
    d, f = w[0].shape[1:]
    n, chunks = pl.cdiv(f, FC), g.shape[1]
    wide = pl.BlockSpec((None, d, FC), lambda c: (1 - (c + start) // n, 0, lax.rem(c + start, n)))
    tall = pl.BlockSpec((None, FC, d), lambda c: (1 - (c + start) // n, lax.rem(c + start, n), 0))
    blocks = [wide, wide, tall]
    gblock = pl.BlockSpec((8, None, 3, g.shape[3], FC), lambda c: (0, c, 0, 0, 0))
    size = 3 * d * FC * chunks
    return pl.pallas_call(
        functools.partial(adamw_body, sum(one.size for one in w)),
        grid=(chunks,),
        in_specs=[once((8, 128)), gblock, *blocks * 3] + [pl.BlockSpec(memory_space=pl.ANY)] * len(done),
        out_specs=blocks * 3,
        out_shape=[jax.ShapeDtypeStruct(o.shape, o.dtype) for o in (*w, *m, *v)],
        input_output_aliases={11 + i: i for i in range(len(done))},
        compiler_params=params(),
        cost_estimate=pl.CostEstimate(flops=120 * size, bytes_accessed=22 * size, transcendentals=size),
        name="adamw",
    )(squares, g, *w, *m, *v, *done)


def solution(mesh):
    def step(x, dy, *arrays):
        weights, m, v = (arrays[i : i + 3] for i in (0, 3, 6))
        x, dy = x[0], dy[0]
        gate, up, h = forward(0, x, *weights)
        whole, one, two, squares = middle(h, x, dy, gate, up, *weights, STARTS)
        parts = [(0, whole), (STARTS[0], lax.all_gather(one, "dp")), (STARTS[1], lax.all_gather(two, "dp"))]
        new = ()
        for start, part in parts:
            new = adamw(start, squares, part, weights, m, v, new)
        return tuple(new)

    return jax.shard_map(
        step,
        mesh=mesh,
        in_specs=(P(("rep", "dp"), None, None),) * 2 + (P(None, None, None),) * 9,
        out_specs=(P("rep", None, None),) * 9,
        check_vma=False,
    )
```
